32 devices in a mesh: dp: 2 (over core), fsdp: 16 (over z, y, x).
Axes of the slice: x: 2, y: 2, z: 4, core: 2. Of those that a mesh axis runs over, the one named last changes fastest.
Arguments:
- tokens: bfloat16 [8192, 4096], P(('dp', 'fsdp')), may hold values from -6 to 6
- block_codes: bfloat16 [256, 128, 128], P('fsdp'), may hold values from -4 to 4
- scales: float32 [256], P('fsdp'), may hold values from 0.008 to 0.03
- counts: int32 [16], replicated, may hold values from 0 to 16, as said below
- cotangent: bfloat16 [8192, 512], P(('dp', 'fsdp')), may hold values from -6 to 6
Outputs:
- projected: bfloat16 [8192, 512], P(('dp', 'fsdp'))
- token_grad: bfloat16 [8192, 4096], P(('dp', 'fsdp'))
- block_grad: bfloat16 [256, 128, 128], P('fsdp')
The draws below stay inside these ranges and needn't reach their ends.
Inputs may be any that keep to these rules, and one draw needn't show every extreme that they name: counts sum to 128; each is at most 16, and some owner has exactly 16 and some none; slots past an owner's count hold values that are not used.
All inputs are finite; a program needn't handle non-finite values.
Results may differ from the reference program's by a relative error of at most 0.009.
Values may be sent and summed in bfloat16 or wider, within the bound.
A program may use at most 128 MiB of HBM per device.

```python
import math
import jax
import jax.numpy as jnp
from jax import lax

D = 4096
KC = 512
TILE = 128
TOKENS = 8192
NBLK = 128
MEAN = 8
MOST = 16
N_FSDP = 16


def draw_counts(key, part):
    shuffled = jax.random.permutation(jax.random.fold_in(key, 11), N_FSDP)
    amounts = jax.random.randint(jax.random.fold_in(key, 12), (N_FSDP // 2,), 0, MEAN + 1)
    amounts = amounts.at[0].set(MEAN)
    shifts = jnp.zeros((N_FSDP,), jnp.int32)
    shifts = shifts.at[shuffled[0::2]].set(amounts).at[shuffled[1::2]].set(-amounts)
    return (MEAN + shifts).astype(jnp.int32)


def strengthened(values, own_key, source, target, blocks, factor):
    owner, partner = [(jnp.arange(values.shape[dim]) // (values.shape[dim] // blocks)).reshape([-1 if axis == dim else 1 for axis in range(values.ndim)]) for dim in (source, target)]
    chosen = jax.random.permutation(own_key, blocks)[partner]
    strong = (owner == chosen) | (owner == (partner + blocks // 2) % blocks)
    return jnp.where(strong, factor * values, values)


def steps_of(own_key, shape, split, low, high):
    loudness = 1.0
    for dim, parts in split:
        steps = jax.random.uniform(jax.random.fold_in(jax.random.fold_in(own_key, 6), dim), (parts,), jnp.float32, low / len(split), high / len(split))
        loudness = loudness * jnp.repeat(jnp.exp(steps), shape[dim] // parts).reshape((-1,) + (1,) * (len(shape) - 1 - dim))
    return loudness


def normal_values(own_key, shape, scale, most, cuts=(), held_as=jnp.bfloat16):
    loudness = steps_of(own_key, shape, cuts, -0.22, 0.18) if cuts else 1.0
    values = jax.random.normal(own_key, shape, jnp.float32) * scale * loudness
    return jnp.minimum(jnp.maximum(values, -most), most).astype(held_as)


def heavy_noise(stream_key, extent, width, limit, cuts, heavy, kind=jnp.bfloat16):
    values = width * jax.random.normal(stream_key, extent, jnp.float32)
    if cuts:
        values = values * steps_of(stream_key, extent, cuts, -0.22, 0.18)
    return jnp.clip(strengthened(values, jax.random.fold_in(stream_key, 3), *heavy), -limit, limit).astype(kind)


def setup_inputs(seed: int = 0) -> dict:
    arg_keys = jax.random.split(jax.random.key(seed), 6)
    tokens = heavy_noise(arg_keys[0], (TOKENS, D), 1.0, 6.0, ((0, 32),), (0, 1, 32, 2.75))
    block_codes = normal_values(arg_keys[1], (N_FSDP * MOST, TILE, TILE), 1.0, 4.0, ((0, 16),))
    scales = jnp.clip(jnp.exp(math.log(0.03) - 1.3217558 * jax.random.uniform(arg_keys[2], (N_FSDP * MOST,), jnp.float32) ** steps_of(arg_keys[2], (N_FSDP * MOST,), ((0, 16),), -0.2, 0.2)), 0.008, 0.03)
    counts = draw_counts(jax.random.fold_in(arg_keys[5], 71), 0)
    cotangent = normal_values(arg_keys[4], (TOKENS, KC), 1.0, 6.0, ((0, 32),))
    return {"tokens": tokens, "block_codes": block_codes, "scales": scales, "counts": counts, "cotangent": cotangent}


def block_index(counts):
    run_ends = jnp.cumsum(counts).astype(jnp.int32)
    offsets = (run_ends - counts).astype(jnp.int32)
    block_ids = jnp.arange(NBLK, dtype=jnp.int32)
    owners = lax.optimization_barrier(jnp.sum((run_ends[None, :] <= block_ids[:, None]).astype(jnp.int32), axis=1))
    matched = owners[:, None] == jnp.arange(N_FSDP, dtype=jnp.int32)[None, :]
    run_start = lax.optimization_barrier(jnp.sum(jnp.where(matched, offsets[None, :], 0), axis=1)).astype(jnp.int32)
    source_ids = (owners * MOST + block_ids - run_start).astype(jnp.int32)
    return (offsets, source_ids)

def reference(tokens, block_codes, scales, counts, cotangent):
    offsets, source_ids = block_index(counts)
    blocks = block_codes[source_ids].astype(jnp.float32) * scales[source_ids][:, None, None]
    blocks = blocks.astype(jnp.bfloat16)
    weight = blocks.reshape(D // TILE, KC // TILE, TILE, TILE).transpose(0, 2, 1, 3).reshape(D, KC)
    projected = jnp.dot(tokens, weight, preferred_element_type=jnp.float32).astype(jnp.bfloat16)
    token_grad = jnp.dot(cotangent, weight.T, preferred_element_type=jnp.float32).astype(jnp.bfloat16)
    grad = jnp.dot(tokens.T, cotangent, preferred_element_type=jnp.float32) * (1.0 / math.sqrt(TOKENS))
    grad_blocks = grad.reshape(D // TILE, TILE, KC // TILE, TILE).transpose(0, 2, 1, 3).reshape(NBLK, TILE, TILE)
    slot_ids = jnp.arange(N_FSDP * MOST, dtype=jnp.int32)
    owner_of = slot_ids // MOST
    within = slot_ids % MOST
    wanted = (offsets[owner_of] + within).astype(jnp.int32)
    is_valid = within < counts[owner_of]
    picked = grad_blocks[jnp.clip(wanted, 0, NBLK - 1)]
    block_grad = jnp.where(is_valid[:, None, None], picked, jnp.float32(0.0)).astype(jnp.bfloat16)
    return (projected, token_grad, block_grad)
```

```python
import functools
import math
import types

import jax
import jax.numpy as jnp
from jax import lax
from jax.experimental import pallas as pl
from jax.experimental.pallas import tpu as pltpu
from jax.sharding import PartitionSpec as P

MESH = pl.DeviceIdType.MESH
F32 = jnp.float32
BF16 = jnp.bfloat16

PLANE = 4
CORES = 2
GROUP = PLANE * CORES
CHUNKS = 4


def kernel(names, owners, slots, scale, *refs):
    r = types.SimpleNamespace(**dict(zip(names, refs)))
    planes = owners // PLANE
    h = lax.axis_index("dp")
    me = lax.axis_index("fsdp")
    z, c = me // PLANE, me % PLANE
    y, x = c // 2, c % 2
    oy, ox = 1 - y, 1 - x
    most, tile = r.codes_v.shape[0], r.codes_v.shape[1]
    span = r.own_v.shape[1]
    part = span // 2
    places = CHUNKS * span
    blocks = places * GROUP
    period = GROUP * slots
    chunk_blocks = span * GROUP
    plane_most = PLANE * most
    width = r.tok_v.shape[2]
    first, last = pl.ds(0, part), pl.ds(part, span - part)

    x_dev = (h, z * PLANE + 2 * y + ox)
    y_dev = (h, z * PLANE + 2 * oy + x)
    d_dev = (h, z * PLANE + 2 * oy + ox)
    partner = (1 - h, me)

    def z_dev(d):
        return (h, ((z + 1 - 2 * d + planes) % planes) * PLANE + c)

    def remote(src, dst, send, recv, device):
        return pltpu.make_async_remote_copy(
            src_ref=src, dst_ref=dst, send_sem=send, recv_sem=recv, device_id=device, device_id_type=MESH
        )

    ends = []

    def guarded(conditions, act):
        if conditions:
            pl.when(conditions[0])(lambda: guarded(conditions[1:], act))
        else:
            act()

    def go(copy, when=()):
        guarded(when, copy.start)
        ends.append(lambda: guarded(when, copy.wait_send))
        return copy

    local = [
        pltpu.make_async_copy(r.counts_h, r.counts_s, r.in_sems.at[0]),
        pltpu.make_async_copy(r.scales_h, r.scales_s, r.in_sems.at[1]),
        pltpu.make_async_copy(r.codes_h, r.codes_v, r.in_sems.at[2]),
        pltpu.make_async_copy(r.cot_h, r.cot_v, r.in_sems.at[3]),
    ]
    tok_in = [
        pltpu.make_async_copy(
            r.tok_h.at[:, pl.ds(k * width, width)], r.tok_v.at[k], r.tok_sems.at[k]
        )
        for k in range(CHUNKS)
    ]
    for copy in local + tok_in:
        copy.start()

    barrier = pltpu.get_barrier_semaphore()
    for peer in (x_dev, y_dev, d_dev, partner):
        pl.semaphore_signal(barrier, inc=1, device_id=peer, device_id_type=MESH)
    has_up, has_down = z < planes - 1, z > 0

    @pl.when(has_up)
    def _():
        pl.semaphore_signal(barrier, inc=1, device_id=z_dev(0), device_id_type=MESH)

    @pl.when(has_down)
    def _():
        pl.semaphore_signal(barrier, inc=1, device_id=z_dev(1), device_id_type=MESH)

    for copy in local[:3]:
        copy.wait()
    pl.semaphore_wait(barrier, 4 + jnp.where(has_up, 1, 0) + jnp.where(has_down, 1, 0))

    base, run = 0, [0] * PLANE
    for d in range(owners):
        count = r.counts_s[d]
        base = base + jnp.where(d < z * PLANE, count, 0)
        run[d % PLANE] = run[d % PLANE] + jnp.where(d // PLANE == z, count, 0)
    starts = [base]
    for i in range(PLANE):
        starts.append(starts[-1] + run[i])
    plane_end = starts[PLANE]

    def pick(values, index):
        total = values[0]
        for i in range(1, len(values)):
            total = jnp.where(index == i, values[i], total)
        return total

    my_off = pick(starts[:PLANE], c)
    my_count = pick(run, c)

    p = (2 * z) // planes

    def far_chunk(j):
        return (j + (CHUNKS // 2) * (1 - p)) % CHUNKS

    def near_chunk(j):
        return (j + (CHUNKS // 2) * p) % CHUNKS

    behind = (z, planes - 1 - z)

    def ahead(d, q):
        return q if d == 0 else CHUNKS - 1 - q

    def w_has_recv(d, q):
        return (ahead(d, q) * chunk_blocks < behind[d] * plane_most,)

    def w_has_send(d, q):
        v = behind[d]
        return (v < planes - 1, ahead(d, q) * chunk_blocks < (v + 1) * plane_most)

    def g_has_recv(d, q):
        v = behind[d]
        return (v > 0, ahead(d, CHUNKS - 1 - q) * chunk_blocks < (planes - v) * plane_most)

    def g_has_send(d, q):
        return (ahead(d, CHUNKS - 1 - q) * chunk_blocks < (planes - 1 - behind[d]) * plane_most,)

    def place_block(q, i):
        return (q * span + i) * GROUP + h * PLANE + c

    mates = [(y, x), (y, ox), (oy, x), (oy, ox)]
    mate_devs = [None, x_dev, y_dev, d_dev]

    def scatter():
        for k, (ty, tx) in enumerate(mates):
            target = 2 * ty + tx
            for s in range(slots):
                t = lax.rem(s * GROUP + h * PLANE + target - my_off + blocks, period)
                t = jnp.minimum(t, most - 1)
                block = (r.codes_v[t].astype(F32) * r.scales_s[t]).astype(BF16)
                if k == 0:
                    r.sc_recv[c, s] = block
                else:
                    r.sc_send[k, s] = block
        for k in range(1, PLANE):
            go(scatter_copy(k))

    def scatter_copy(k):
        return remote(r.sc_send.at[k], r.sc_recv.at[c], r.sc_sems.at[0, k], r.sc_sems.at[1, k], mate_devs[k])

    def gather_own():
        for k in range(1, PLANE):
            scatter_copy(k).wait_recv()
        for i in range(PLANE):
            r.sc_loc[i * slots : (i + 1) * slots] = r.sc_recv[i]
        for q in range(CHUNKS):
            for i in range(span):
                b = place_block(q, i)
                owner = 0
                for e in starts[1:PLANE]:
                    owner = owner + jnp.where(b >= e, 1, 0)
                r.own_v[q, i] = r.sc_loc[owner * slots + (q * span + i) % slots]

    def w_task(d, q, when):
        copy = remote(r.w_send.at[d, q], r.w_recv.at[d, q], r.wz_sems.at[0, d, q], r.wz_sems.at[1, d, q], z_dev(d))

        guarded(when + w_has_recv(d, q), copy.wait_recv)

        def merge():
            for i in range(span):
                b = place_block(q, i)
                other = b < base if d == 0 else b >= plane_end
                r.w_send[d, q, i] = jnp.where(other, r.w_recv[d, q, i], r.own_v[q, i])

        sends = when + w_has_send(d, q)
        guarded(sends, merge)
        go(copy, sends)

    def line_order(d, j):
        return (j + CHUNKS // 2) % CHUNKS if d == 0 else j

    def w_primary(j):
        for d in range(2):
            w_task(d, line_order(d, (j + CHUNKS // 2) % CHUNKS), (behind[d] == 0,))
            w_task(d, line_order(d, j), (p == d, behind[d] > 0))

    def w_secondary(j):
        for d in range(2):
            w_task(d, line_order(d, j), (p == 1 - d,))

    def push(place, k, j):
        return remote(place, place, r.fw_sems.at[0, k, j], r.fw_sems.at[1, k, j], partner)

    def gather_copy(place, k, j, device):
        return remote(place, place, r.ag_sems.at[0, k, j], r.ag_sems.at[1, k, j], device)

    def w_final(j):
        q = near_chunk(j)
        w_secondary(j)
        for i in range(span):
            b = place_block(q, i)
            r.w_all[h, q, y, x, i] = jnp.where(
                b < base, r.w_recv[0, q, i], jnp.where(b >= plane_end, r.w_recv[1, q, i], r.own_v[q, i])
            )
        place = r.w_all.at[h, q, y, x]
        go(gather_copy(place, 0, j, x_dev))
        go(gather_copy(place, 1, j, y_dev))
        go(push(place, 0, j))

    def w_forward(j):
        q = near_chunk(j)
        place = r.w_all.at[h, q, y, ox]
        gather_copy(place, 0, j, x_dev).wait_recv()
        go(gather_copy(r.w_all.at[h, q, y, ox, first], 2, j, y_dev))
        go(push(place, 1, j))
        place = r.w_all.at[h, q, oy, x]
        gather_copy(place, 1, j, y_dev).wait_recv()
        go(gather_copy(r.w_all.at[h, q, oy, x, last], 3, j, x_dev))
        go(push(place, 2, j))

    def w_diagonal(j):
        q = near_chunk(j)
        gather_copy(r.w_all.at[h, q, oy, ox, first], 2, j, y_dev).wait_recv()
        gather_copy(r.w_all.at[h, q, oy, ox, last], 3, j, x_dev).wait_recv()
        go(push(r.w_all.at[h, q, oy, ox], 3, j))

    depth = r.w_mat.shape[0]
    row_tiles = depth // tile

    def products(j):
        q = near_chunk(j)
        for k, (ty, tx) in enumerate(mates):
            push(r.w_all.at[1 - h, q, ty, tx], k, j).wait_recv()
        for rr in range(row_tiles):
            for cc in range(PLANE):
                r.w_mat[rr * tile : (rr + 1) * tile, cc * tile : (cc + 1) * tile] = r.w_all[
                    rr % CORES, q, cc // 2, cc % 2, rr // CORES
                ]
        weight = r.w_mat[...]
        term = jnp.dot(r.tok_v[q], weight, preferred_element_type=F32)
        if j == 0:
            r.acc[...] = term
        elif j < CHUNKS - 1:
            r.acc[...] += term
        else:
            r.proj[...] = (r.acc[...] + term).astype(BF16)
        r.tg[:, pl.ds(pl.multiple_of(q * depth, depth), depth)] = lax.dot_general(
            r.cot_v[...], weight, (((1,), (1,)), ((), ())), preferred_element_type=F32
        ).astype(BF16)

    steps = 2
    sub = depth // steps

    def pair_copy(j):
        q = far_chunk(j)
        return remote(r.g_terms.at[1 - h, q], r.g_pair.at[q], r.pair_sems.at[0, j], r.pair_sems.at[1, j], partner)

    def terms(j):
        q = far_chunk(j)
        for g in range(steps):
            value = lax.dot_general(
                r.tok_v[q, :, g * sub : (g + 1) * sub], r.cot_v[...], (((0,), (0,)), ((), ())),
                preferred_element_type=F32,
            )
            value = (value * scale).astype(BF16)
            for rr in range(sub // tile):
                row = g * (sub // tile) + rr
                for cc in range(PLANE):
                    r.g_terms[row % CORES, q, cc // 2, cc % 2, row // CORES] = value[
                        rr * tile : (rr + 1) * tile, cc * tile : (cc + 1) * tile
                    ]
        go(pair_copy(j))

    def pair_sum(j):
        q = far_chunk(j)
        pair_copy(j).wait_recv()

        for a in range(2):
            for b in range(2):
                r.g_sum[q, a, b] = (r.g_terms[h, q, a, b].astype(F32) + r.g_pair[q, a, b].astype(F32)).astype(BF16)

    def rs_one(j):
        q = far_chunk(j)
        return [
            remote(r.g_sum.at[q, oy, :, first], r.r1a.at[q], r.rs_sems.at[0, 0, j], r.rs_sems.at[1, 0, j], y_dev),
            remote(r.g_sum.at[q, :, ox, last], r.r1b.at[q], r.rs_sems.at[0, 1, j], r.rs_sems.at[1, 1, j], x_dev),
        ]

    def rs_two(j):
        q = far_chunk(j)
        return [
            remote(r.s2a.at[q], r.r2a.at[q], r.rs_sems.at[0, 2, j], r.rs_sems.at[1, 2, j], x_dev),
            remote(r.s2b.at[q], r.r2b.at[q], r.rs_sems.at[0, 3, j], r.rs_sems.at[1, 3, j], y_dev),
        ]

    def reduce_one(j):
        for copy in rs_one(j):
            go(copy)

    def reduce_two(j):
        q = far_chunk(j)
        one, two = rs_one(j), rs_two(j)
        one[0].wait_recv()
        r.s2a[q] = (r.g_sum[q, y, ox, first].astype(F32) + r.r1a[q, ox].astype(F32)).astype(BF16)
        go(two[0])
        one[1].wait_recv()
        r.s2b[q] = (r.g_sum[q, oy, x, last].astype(F32) + r.r1b[q, oy].astype(F32)).astype(BF16)
        go(two[1])

    def plane_sum(j):
        q = far_chunk(j)
        two = rs_two(j)
        two[0].wait_recv()
        r.g_plane[q, first] = (
            r.g_sum[q, y, x, first].astype(F32) + r.r1a[q, x].astype(F32) + r.r2a[q].astype(F32)
        )
        two[1].wait_recv()
        r.g_plane[q, last] = (
            r.g_sum[q, y, x, last].astype(F32) + r.r1b[q, y].astype(F32) + r.r2b[q].astype(F32)
        )

    def behind_sum(d, q):
        return jnp.where(behind[d] > 0, r.gz_recv[d, q].astype(F32), 0.0)

    def g_task(d, q, when):
        copy = remote(r.gz_send.at[d, q], r.gz_recv.at[d, q], r.gz_sems.at[0, d, q], r.gz_sems.at[1, d, q], z_dev(d))

        guarded(when + g_has_recv(d, q), copy.wait_recv)

        def add():
            r.gz_send[d, q] = (r.g_plane[q] + behind_sum(d, q)).astype(BF16)

        sends = when + g_has_send(d, q)
        guarded(sends, add)
        go(copy, sends)

    def g_primary(slot):
        for d in range(2):
            if slot < CHUNKS:
                g_task(d, line_order(d, slot), (behind[d] == 0,))
            if slot > 0:
                g_task(d, line_order(d, slot - 1), (p == d, behind[d] > 0))

    def g_secondary(j):
        for d in range(2):
            g_task(d, line_order(d, j), (p == 1 - d,))
        q = near_chunk(j)
        r.g_full[pl.ds(q * span, span)] = (r.g_plane[q] + behind_sum(0, q) + behind_sum(1, q)).astype(BF16)

    def owner_copy(k):
        return remote(r.fs_send.at[k], r.fs_all.at[h, c], r.fs_sems.at[0, k], r.fs_sems.at[1, k], mate_devs[k])

    def give(k):
        ty, tx = mates[k]
        place = r.fs_all.at[h, 2 * ty + tx]
        return remote(place, place, r.fp_sems.at[0, k], r.fp_sems.at[1, k], partner)

    def to_owners():
        for k in (3, 1, 2, 0):
            ty, tx = mates[k]
            off = pick(starts[:PLANE], 2 * ty + tx)
            for s in range(slots):
                t = lax.rem(s * GROUP + h * PLANE + c - off + blocks, period)
                m = jnp.minimum(lax.div(off + t, GROUP), places - 1)
                block = r.g_full[m]
                if k == 0:
                    r.fs_all[h, c, s] = block
                else:
                    r.fs_send[k, s] = block
        for k in (3, 1, 2):
            go(owner_copy(k))
        go(give(0))

    def finish():
        for k in (1, 2, 3):
            owner_copy(k).wait_recv()
            go(give(k))
        for k in range(PLANE):
            ty, tx = mates[k]
            place = r.fs_all.at[1 - h, 2 * ty + tx]
            remote(place, place, r.fp_sems.at[0, k], r.fp_sems.at[1, k], partner).wait_recv()
        for k in range(CORES * PLANE):
            r.fs_loc[k * slots : (k + 1) * slots] = r.fs_all[k // PLANE, k % PLANE]
        for j in range(most):
            b = my_off + j
            block = r.fs_loc[lax.rem(b, GROUP) * slots + lax.rem(lax.div(b, GROUP), slots)]
            r.out[j] = jnp.where(j < my_count, block, jnp.zeros_like(block))

    scatter()
    local[3].wait()
    for copy in tok_in:
        copy.wait()
    for j in range(CHUNKS):
        terms(j)
    pair_sum(0)
    reduce_one(0)
    pair_sum(1)
    reduce_one(1)
    gather_own()
    w_primary(0)
    w_primary(1)
    pair_sum(2)
    pair_sum(3)
    reduce_two(0)
    reduce_one(2)
    w_primary(2)
    reduce_two(1)
    reduce_one(3)
    plane_sum(0)
    g_primary(0)
    w_primary(3)
    w_final(0)
    reduce_two(2)
    plane_sum(1)
    g_primary(1)
    w_final(1)
    w_forward(0)
    reduce_two(3)
    plane_sum(2)
    g_primary(2)
    w_final(2)
    w_forward(1)
    w_diagonal(0)
    plane_sum(3)
    g_primary(3)
    w_final(3)
    g_primary(4)
    g_secondary(0)
    w_forward(2)
    w_diagonal(1)
    products(0)
    g_secondary(1)
    w_forward(3)
    g_secondary(2)
    g_secondary(3)
    to_owners()
    w_diagonal(2)
    products(1)
    w_diagonal(3)
    products(2)
    finish()
    products(3)
    for end in ends:
        end()


def body(tokens, block_codes, scales, counts, cotangent):
    owners = lax.axis_size("fsdp")
    most, tile = block_codes.shape[0], block_codes.shape[1]
    local_tokens, width = tokens.shape
    key_width = cotangent.shape[1]
    blocks = (width // tile) * (key_width // tile)
    total_tokens = local_tokens * lax.axis_size("dp") * owners
    slots = -(-most // GROUP)
    span = blocks // (GROUP * CHUNKS)
    depth = width // CHUNKS
    assert lax.axis_size("dp") == CORES and owners % PLANE == 0 and key_width == PLANE * tile
    assert span * GROUP * CHUNKS == blocks and span % 2 == 0 and span % slots == 0

    dma = pltpu.SemaphoreType.DMA
    vmem = pl.BlockSpec(memory_space=pltpu.VMEM)
    hbm = pl.BlockSpec(memory_space=pltpu.HBM)

    def held(*shape, kind=BF16):
        return pltpu.VMEM(shape + (tile, tile), kind)

    half, places = span // 2, span * CHUNKS
    scratch = {
        "counts_s": pltpu.SMEM(counts.shape, jnp.int32),
        "scales_s": pltpu.SMEM(scales.shape, F32),
        "codes_v": pltpu.VMEM(block_codes.shape, BF16),
        "cot_v": pltpu.VMEM(cotangent.shape, BF16),
        "tok_v": pltpu.VMEM((CHUNKS, local_tokens, depth), BF16),
        "sc_send": held(PLANE, slots),
        "sc_recv": held(PLANE, slots),
        "sc_loc": held(PLANE * slots),
        "fs_loc": held(CORES * PLANE * slots),
        "own_v": held(CHUNKS, span),
        "w_send": held(2, CHUNKS, span),
        "w_recv": held(2, CHUNKS, span),
        "w_all": held(CORES, CHUNKS, 2, 2, span),
        "w_mat": pltpu.VMEM((depth, key_width), BF16),
        "acc": pltpu.VMEM((local_tokens, key_width), F32),
        "g_terms": held(CORES, CHUNKS, 2, 2, span),
        "g_pair": held(CHUNKS, 2, 2, span),
        "g_sum": held(CHUNKS, 2, 2, span),
        "r1a": held(CHUNKS, 2, half),
        "r1b": held(CHUNKS, 2, half),
        "s2a": held(CHUNKS, half),
        "s2b": held(CHUNKS, half),
        "r2a": held(CHUNKS, half),
        "r2b": held(CHUNKS, half),
        "g_plane": held(CHUNKS, span, kind=F32),
        "gz_send": held(2, CHUNKS, span),
        "gz_recv": held(2, CHUNKS, span),
        "g_full": held(places),
        "fs_send": held(PLANE, slots),
        "fs_all": held(CORES, PLANE, slots),
        "in_sems": dma((4,)),
        "tok_sems": dma((CHUNKS,)),
        "sc_sems": dma((2, PLANE)),
        "wz_sems": dma((2, 2, CHUNKS)),
        "ag_sems": dma((2, 4, CHUNKS)),
        "fw_sems": dma((2, 4, CHUNKS)),
        "pair_sems": dma((2, CHUNKS)),
        "rs_sems": dma((2, 4, CHUNKS)),
        "gz_sems": dma((2, 2, CHUNKS)),
        "fs_sems": dma((2, PLANE)),
        "fp_sems": dma((2, PLANE)),
    }
    names = ["counts_h", "scales_h", "codes_h", "tok_h", "cot_h", "proj", "tg", "out"] + list(scratch)
    return tuple(pl.pallas_call(
        functools.partial(kernel, names, owners, slots, 1.0 / math.sqrt(total_tokens)),
        in_specs=[hbm] * 5,
        out_specs=[vmem, vmem, vmem],
        out_shape=[
            jax.ShapeDtypeStruct((local_tokens, key_width), BF16),
            jax.ShapeDtypeStruct((local_tokens, width), BF16),
            jax.ShapeDtypeStruct((most, tile, tile), BF16),
        ],
        scratch_shapes=list(scratch.values()),
        compiler_params=pltpu.CompilerParams(
            collective_id=0, has_side_effects=True, vmem_limit_bytes=56 * 1024 * 1024
        ),
    )(counts, scales, block_codes, tokens, cotangent))


def solution(mesh):
    return jax.shard_map(
        body,
        mesh=mesh,
        in_specs=(
            P(("dp", "fsdp"), None),
            P("fsdp", None, None),
            P("fsdp"),
            P(),
            P(("dp", "fsdp"), None),
        ),
        out_specs=(P(("dp", "fsdp"), None), P(("dp", "fsdp"), None), P("fsdp", None, None)),
        check_vma=False,
    )
```

```python
import functools
import math
import types

import jax
import jax.numpy as jnp
from jax import lax
from jax.experimental import pallas as pl
from jax.experimental.pallas import tpu as pltpu
from jax.sharding import PartitionSpec as P

MESH = pl.DeviceIdType.MESH
F32 = jnp.float32
BF16 = jnp.bfloat16

PLANE = 4
CORES = 2
GROUP = PLANE * CORES
CHUNKS = 4


def kernel(names, owners, slots, scale, *refs):
    r = types.SimpleNamespace(**dict(zip(names, refs)))
    planes = owners // PLANE
    h = lax.axis_index("dp")
    me = lax.axis_index("fsdp")
    z, c = me // PLANE, me % PLANE
    y, x = c // 2, c % 2
    oy, ox = 1 - y, 1 - x
    most, tile = r.codes_v.shape[0], r.codes_v.shape[1]
    span = r.own_v.shape[1]
    part = span // 2
    places = CHUNKS * span
    blocks = places * GROUP
    period = GROUP * slots
    chunk_blocks = span * GROUP
    plane_most = PLANE * most
    width = r.tok_v.shape[2]
    first, last = pl.ds(0, part), pl.ds(part, span - part)

    x_dev = (h, z * PLANE + 2 * y + ox)
    y_dev = (h, z * PLANE + 2 * oy + x)
    d_dev = (h, z * PLANE + 2 * oy + ox)
    partner = (1 - h, me)

    def z_dev(d):
        return (h, ((z + 1 - 2 * d + planes) % planes) * PLANE + c)

    def remote(src, dst, send, recv, device):
        return pltpu.make_async_remote_copy(
            src_ref=src, dst_ref=dst, send_sem=send, recv_sem=recv, device_id=device, device_id_type=MESH
        )

    ends = []

    def guarded(conditions, act):
        if conditions:
            pl.when(conditions[0])(lambda: guarded(conditions[1:], act))
        else:
            act()

    def go(copy, when=()):
        guarded(when, copy.start)
        ends.append(lambda: guarded(when, copy.wait_send))
        return copy

    local = [
        pltpu.make_async_copy(r.counts_h, r.counts_s, r.in_sems.at[0]),
        pltpu.make_async_copy(r.scales_h, r.scales_s, r.in_sems.at[1]),
        pltpu.make_async_copy(r.codes_h, r.codes_v, r.in_sems.at[2]),
        pltpu.make_async_copy(r.cot_h, r.cot_v, r.in_sems.at[3]),
    ]
    tok_in = [
        pltpu.make_async_copy(
            r.tok_h.at[:, pl.ds(k * width, width)], r.tok_v.at[k], r.tok_sems.at[k]
        )
        for k in range(CHUNKS)
    ]
    for copy in local + tok_in:
        copy.start()

    barrier = pltpu.get_barrier_semaphore()
    for peer in (x_dev, y_dev, d_dev, partner):
        pl.semaphore_signal(barrier, inc=1, device_id=peer, device_id_type=MESH)
    has_up, has_down = z < planes - 1, z > 0

    @pl.when(has_up)
    def _():
        pl.semaphore_signal(barrier, inc=1, device_id=z_dev(0), device_id_type=MESH)

    @pl.when(has_down)
    def _():
        pl.semaphore_signal(barrier, inc=1, device_id=z_dev(1), device_id_type=MESH)

    for copy in local[:3]:
        copy.wait()
    pl.semaphore_wait(barrier, 4 + jnp.where(has_up, 1, 0) + jnp.where(has_down, 1, 0))

    base, run = 0, [0] * PLANE
    for d in range(owners):
        count = r.counts_s[d]
        base = base + jnp.where(d < z * PLANE, count, 0)
        run[d % PLANE] = run[d % PLANE] + jnp.where(d // PLANE == z, count, 0)
    starts = [base]
    for i in range(PLANE):
        starts.append(starts[-1] + run[i])
    plane_end = starts[PLANE]

    def pick(values, index):
        total = values[0]
        for i in range(1, len(values)):
            total = jnp.where(index == i, values[i], total)
        return total

    my_off = pick(starts[:PLANE], c)
    my_count = pick(run, c)

    p = (2 * z) // planes

    def far_chunk(j):
        return (j + (CHUNKS // 2) * (1 - p)) % CHUNKS

    def near_chunk(j):
        return (j + (CHUNKS // 2) * p) % CHUNKS

    behind = (z, planes - 1 - z)

    def ahead(d, q):
        return q if d == 0 else CHUNKS - 1 - q

    def w_has_recv(d, q):
        return (ahead(d, q) * chunk_blocks < behind[d] * plane_most,)

    def w_has_send(d, q):
        v = behind[d]
        return (v < planes - 1, ahead(d, q) * chunk_blocks < (v + 1) * plane_most)

    def g_has_recv(d, q):
        v = behind[d]
        return (v > 0, ahead(d, CHUNKS - 1 - q) * chunk_blocks < (planes - v) * plane_most)

    def g_has_send(d, q):
        return (ahead(d, CHUNKS - 1 - q) * chunk_blocks < (planes - 1 - behind[d]) * plane_most,)

    def place_block(q, i):
        return (q * span + i) * GROUP + h * PLANE + c

    mates = [(y, x), (y, ox), (oy, x), (oy, ox)]
    mate_devs = [None, x_dev, y_dev, d_dev]

    def scatter():
        for k, (ty, tx) in enumerate(mates):
            target = 2 * ty + tx
            for s in range(slots):
                t = lax.rem(s * GROUP + h * PLANE + target - my_off + blocks, period)
                t = jnp.minimum(t, most - 1)
                block = (r.codes_v[t].astype(F32) * r.scales_s[t]).astype(BF16)
                if k == 0:
                    r.sc_recv[c, s] = block
                else:
                    r.sc_send[k, s] = block
        for k in range(1, PLANE):
            go(scatter_copy(k))

    def scatter_copy(k):
        return remote(r.sc_send.at[k], r.sc_recv.at[c], r.sc_sems.at[0, k], r.sc_sems.at[1, k], mate_devs[k])

    def gather_own():
        for k in range(1, PLANE):
            scatter_copy(k).wait_recv()
        for i in range(PLANE):
            r.sc_loc[i * slots : (i + 1) * slots] = r.sc_recv[i]
        for q in range(CHUNKS):
            for i in range(span):
                b = place_block(q, i)
                owner = 0
                for e in starts[1:PLANE]:
                    owner = owner + jnp.where(b >= e, 1, 0)
                r.own_v[q, i] = r.sc_loc[owner * slots + (q * span + i) % slots]

    def w_task(d, q, when):
        copy = remote(r.w_send.at[d, q], r.w_recv.at[d, q], r.wz_sems.at[0, d, q], r.wz_sems.at[1, d, q], z_dev(d))

        guarded(when + w_has_recv(d, q), copy.wait_recv)

        def merge():
            for i in range(span):
                b = place_block(q, i)
                other = b < base if d == 0 else b >= plane_end
                r.w_send[d, q, i] = jnp.where(other, r.w_recv[d, q, i], r.own_v[q, i])

        sends = when + w_has_send(d, q)
        guarded(sends, merge)
        go(copy, sends)

    def line_order(d, j):
        return (j + CHUNKS // 2) % CHUNKS if d == 0 else j

    def w_primary(j):
        for d in range(2):
            w_task(d, line_order(d, (j + CHUNKS // 2) % CHUNKS), (behind[d] == 0,))
            w_task(d, line_order(d, j), (p == d, behind[d] > 0))

    def w_middle(j):
        for d in range(2):
            w_task(d, line_order(d, j), (p == 1 - d, behind[d] < planes - 1))

    def w_end(j):
        for d in range(2):
            w_task(d, line_order(d, j), (behind[d] == planes - 1,))

    def push(place, k, j):
        return remote(place, place, r.fw_sems.at[0, k, j], r.fw_sems.at[1, k, j], partner)

    def gather_copy(place, k, j, device):
        return remote(place, place, r.ag_sems.at[0, k, j], r.ag_sems.at[1, k, j], device)

    def w_final(j):
        q = near_chunk(j)
        w_end(j)
        for i in range(span):
            b = place_block(q, i)
            r.w_all[h, q, y, x, i] = jnp.where(
                b < base, r.w_recv[0, q, i], jnp.where(b >= plane_end, r.w_recv[1, q, i], r.own_v[q, i])
            )
        place = r.w_all.at[h, q, y, x]
        go(gather_copy(place, 0, j, x_dev))
        go(gather_copy(place, 1, j, y_dev))
        go(push(place, 0, j))

    def w_forward(j):
        q = near_chunk(j)
        place = r.w_all.at[h, q, y, ox]
        gather_copy(place, 0, j, x_dev).wait_recv()
        go(gather_copy(r.w_all.at[h, q, y, ox, first], 2, j, y_dev))
        go(push(place, 1, j))
        place = r.w_all.at[h, q, oy, x]
        gather_copy(place, 1, j, y_dev).wait_recv()
        go(gather_copy(r.w_all.at[h, q, oy, x, last], 3, j, x_dev))
        go(push(place, 2, j))

    def w_diagonal(j):
        q = near_chunk(j)
        gather_copy(r.w_all.at[h, q, oy, ox, first], 2, j, y_dev).wait_recv()
        gather_copy(r.w_all.at[h, q, oy, ox, last], 3, j, x_dev).wait_recv()
        go(push(r.w_all.at[h, q, oy, ox], 3, j))

    depth = r.w_mat.shape[0]
    row_tiles = depth // tile

    def products(j):
        q = near_chunk(j)
        for k, (ty, tx) in enumerate(mates):
            push(r.w_all.at[1 - h, q, ty, tx], k, j).wait_recv()
        for rr in range(row_tiles):
            for cc in range(PLANE):
                r.w_mat[rr * tile : (rr + 1) * tile, cc * tile : (cc + 1) * tile] = r.w_all[
                    rr % CORES, q, cc // 2, cc % 2, rr // CORES
                ]
        weight = r.w_mat[...]
        term = jnp.dot(r.tok_v[q], weight, preferred_element_type=F32)
        if j == 0:
            r.acc[...] = term
        elif j < CHUNKS - 1:
            r.acc[...] += term
        else:
            r.proj[...] = (r.acc[...] + term).astype(BF16)
        r.tg[:, pl.ds(pl.multiple_of(q * depth, depth), depth)] = lax.dot_general(
            r.cot_v[...], weight, (((1,), (1,)), ((), ())), preferred_element_type=F32
        ).astype(BF16)

    steps = 2
    sub = depth // steps

    def pair_copy(j):
        q = far_chunk(j)
        return remote(r.g_terms.at[1 - h, q], r.g_pair.at[q], r.pair_sems.at[0, j], r.pair_sems.at[1, j], partner)

    def terms(j):
        q = far_chunk(j)
        for g in range(steps):
            value = lax.dot_general(
                r.tok_v[q, :, g * sub : (g + 1) * sub], r.cot_v[...], (((0,), (0,)), ((), ())),
                preferred_element_type=F32,
            )
            value = (value * scale).astype(BF16)
            for rr in range(sub // tile):
                row = g * (sub // tile) + rr
                for cc in range(PLANE):
                    r.g_terms[row % CORES, q, cc // 2, cc % 2, row // CORES] = value[
                        rr * tile : (rr + 1) * tile, cc * tile : (cc + 1) * tile
                    ]
        go(pair_copy(j))

    def pair_sum(j):
        q = far_chunk(j)
        pair_copy(j).wait_recv()

        for a in range(2):
            for b in range(2):
                r.g_sum[q, a, b] = (r.g_terms[h, q, a, b].astype(F32) + r.g_pair[q, a, b].astype(F32)).astype(BF16)

    def rs_one(j):
        q = far_chunk(j)
        return [
            remote(r.g_sum.at[q, oy, :, first], r.r1a.at[q], r.rs_sems.at[0, 0, j], r.rs_sems.at[1, 0, j], y_dev),
            remote(r.g_sum.at[q, :, ox, last], r.r1b.at[q], r.rs_sems.at[0, 1, j], r.rs_sems.at[1, 1, j], x_dev),
        ]

    def rs_two(j):
        q = far_chunk(j)
        return [
            remote(r.s2a.at[q], r.r2a.at[q], r.rs_sems.at[0, 2, j], r.rs_sems.at[1, 2, j], x_dev),
            remote(r.s2b.at[q], r.r2b.at[q], r.rs_sems.at[0, 3, j], r.rs_sems.at[1, 3, j], y_dev),
        ]

    def reduce_one(j):
        for copy in rs_one(j):
            go(copy)

    def reduce_two(j):
        q = far_chunk(j)
        one, two = rs_one(j), rs_two(j)
        one[0].wait_recv()
        r.s2a[q] = (r.g_sum[q, y, ox, first].astype(F32) + r.r1a[q, ox].astype(F32)).astype(BF16)
        go(two[0])
        one[1].wait_recv()
        r.s2b[q] = (r.g_sum[q, oy, x, last].astype(F32) + r.r1b[q, oy].astype(F32)).astype(BF16)
        go(two[1])

    def plane_sum(j):
        q = far_chunk(j)
        two = rs_two(j)
        two[0].wait_recv()
        r.g_plane[q, first] = (
            r.g_sum[q, y, x, first].astype(F32) + r.r1a[q, x].astype(F32) + r.r2a[q].astype(F32)
        )
        two[1].wait_recv()
        r.g_plane[q, last] = (
            r.g_sum[q, y, x, last].astype(F32) + r.r1b[q, y].astype(F32) + r.r2b[q].astype(F32)
        )

    def behind_sum(d, q):
        return jnp.where(behind[d] > 0, r.gz_recv[d, q].astype(F32), 0.0)

    def g_task(d, q, when):
        copy = remote(r.gz_send.at[d, q], r.gz_recv.at[d, q], r.gz_sems.at[0, d, q], r.gz_sems.at[1, d, q], z_dev(d))

        guarded(when + g_has_recv(d, q), copy.wait_recv)

        def add():
            r.gz_send[d, q] = (r.g_plane[q] + behind_sum(d, q)).astype(BF16)

        sends = when + g_has_send(d, q)
        guarded(sends, add)
        go(copy, sends)

    def g_primary(slot):
        for d in range(2):
            if slot < CHUNKS:
                g_task(d, line_order(d, slot), (behind[d] == 0,))
            if slot > 0:
                g_task(d, line_order(d, slot - 1), (p == d, behind[d] > 0))

    def g_middle(j):
        for d in range(2):
            g_task(d, line_order(d, j), (p == 1 - d, behind[d] < planes - 1))

    def g_final(j):
        for d in range(2):
            g_task(d, line_order(d, j), (behind[d] == planes - 1,))
        q = near_chunk(j)
        r.g_full[pl.ds(q * span, span)] = (r.g_plane[q] + behind_sum(0, q) + behind_sum(1, q)).astype(BF16)

    def owner_copy(k):
        return remote(r.fs_send.at[k], r.fs_all.at[h, c], r.fs_sems.at[0, k], r.fs_sems.at[1, k], mate_devs[k])

    def give(k):
        ty, tx = mates[k]
        place = r.fs_all.at[h, 2 * ty + tx]
        return remote(place, place, r.fp_sems.at[0, k], r.fp_sems.at[1, k], partner)

    def to_owners():
        for k in (3, 1, 2, 0):
            ty, tx = mates[k]
            off = pick(starts[:PLANE], 2 * ty + tx)
            for s in range(slots):
                t = lax.rem(s * GROUP + h * PLANE + c - off + blocks, period)
                m = jnp.minimum(lax.div(off + t, GROUP), places - 1)
                block = r.g_full[m]
                if k == 0:
                    r.fs_all[h, c, s] = block
                else:
                    r.fs_send[k, s] = block
        for k in (3, 1, 2):
            go(owner_copy(k))
        go(give(0))

    def finish():
        for k in (1, 2, 3):
            owner_copy(k).wait_recv()
            go(give(k))
        for k in range(PLANE):
            ty, tx = mates[k]
            place = r.fs_all.at[1 - h, 2 * ty + tx]
            remote(place, place, r.fp_sems.at[0, k], r.fp_sems.at[1, k], partner).wait_recv()
        for k in range(CORES * PLANE):
            r.fs_loc[k * slots : (k + 1) * slots] = r.fs_all[k // PLANE, k % PLANE]
        for j in range(most):
            b = my_off + j
            block = r.fs_loc[lax.rem(b, GROUP) * slots + lax.rem(lax.div(b, GROUP), slots)]
            r.out[j] = jnp.where(j < my_count, block, jnp.zeros_like(block))

    scatter()
    local[3].wait()
    for copy in tok_in:
        copy.wait()
    for j in range(CHUNKS):
        terms(j)
    pair_sum(0)
    reduce_one(0)
    pair_sum(1)
    reduce_one(1)
    gather_own()
    w_primary(0)
    w_primary(1)
    pair_sum(2)
    pair_sum(3)
    reduce_two(0)
    reduce_one(2)
    w_primary(2)
    w_middle(0)
    reduce_two(1)
    reduce_one(3)
    w_primary(3)
    plane_sum(0)
    g_primary(0)
    w_middle(1)
    reduce_two(2)
    plane_sum(1)
    g_primary(1)
    w_middle(2)
    w_final(0)
    reduce_two(3)
    plane_sum(2)
    g_primary(2)
    g_middle(0)
    w_middle(3)
    w_final(1)
    plane_sum(3)
    g_middle(1)
    w_final(2)
    w_forward(0)
    g_primary(3)
    w_final(3)
    w_forward(1)
    w_diagonal(0)
    g_primary(4)
    products(0)
    w_diagonal(1)
    w_forward(2)
    products(1)
    g_middle(2)
    g_middle(3)
    g_final(0)
    g_final(1)
    g_final(2)
    g_final(3)
    to_owners()
    w_forward(3)
    w_diagonal(2)
    products(2)
    w_diagonal(3)
    finish()
    products(3)
    for end in ends:
        end()


def store_kernel(proj, tg, out, proj_h, tg_h, out_h, sems):
    copies = [
        pltpu.make_async_copy(src, dst, sems.at[k])
        for k, (src, dst) in enumerate([(tg, tg_h), (out, out_h), (proj, proj_h)])
    ]
    for copy in copies:
        copy.start()
    for copy in copies:
        copy.wait()


def body(tokens, block_codes, scales, counts, cotangent):
    owners = lax.axis_size("fsdp")
    most, tile = block_codes.shape[0], block_codes.shape[1]
    local_tokens, width = tokens.shape
    key_width = cotangent.shape[1]
    blocks = (width // tile) * (key_width // tile)
    total_tokens = local_tokens * lax.axis_size("dp") * owners
    slots = -(-most // GROUP)
    span = blocks // (GROUP * CHUNKS)
    depth = width // CHUNKS
    assert lax.axis_size("dp") == CORES and owners % PLANE == 0 and key_width == PLANE * tile
    assert span * GROUP * CHUNKS == blocks and span % 2 == 0 and span % slots == 0

    dma = pltpu.SemaphoreType.DMA
    vmem = pl.BlockSpec(memory_space=pltpu.VMEM)
    hbm = pl.BlockSpec(memory_space=pltpu.HBM)

    def held(*shape, kind=BF16):
        return pltpu.VMEM(shape + (tile, tile), kind)

    half, places = span // 2, span * CHUNKS
    scratch = {
        "counts_s": pltpu.SMEM(counts.shape, jnp.int32),
        "scales_s": pltpu.SMEM(scales.shape, F32),
        "codes_v": pltpu.VMEM(block_codes.shape, BF16),
        "cot_v": pltpu.VMEM(cotangent.shape, BF16),
        "tok_v": pltpu.VMEM((CHUNKS, local_tokens, depth), BF16),
        "sc_send": held(PLANE, slots),
        "sc_recv": held(PLANE, slots),
        "sc_loc": held(PLANE * slots),
        "fs_loc": held(CORES * PLANE * slots),
        "own_v": held(CHUNKS, span),
        "w_send": held(2, CHUNKS, span),
        "w_recv": held(2, CHUNKS, span),
        "w_all": held(CORES, CHUNKS, 2, 2, span),
        "w_mat": pltpu.VMEM((depth, key_width), BF16),
        "acc": pltpu.VMEM((local_tokens, key_width), F32),
        "g_terms": held(CORES, CHUNKS, 2, 2, span),
        "g_pair": held(CHUNKS, 2, 2, span),
        "g_sum": held(CHUNKS, 2, 2, span),
        "r1a": held(CHUNKS, 2, half),
        "r1b": held(CHUNKS, 2, half),
        "s2a": held(CHUNKS, half),
        "s2b": held(CHUNKS, half),
        "r2a": held(CHUNKS, half),
        "r2b": held(CHUNKS, half),
        "g_plane": held(CHUNKS, span, kind=F32),
        "gz_send": held(2, CHUNKS, span),
        "gz_recv": held(2, CHUNKS, span),
        "g_full": held(places),
        "fs_send": held(PLANE, slots),
        "fs_all": held(CORES, PLANE, slots),
        "in_sems": dma((4,)),
        "tok_sems": dma((CHUNKS,)),
        "sc_sems": dma((2, PLANE)),
        "wz_sems": dma((2, 2, CHUNKS)),
        "ag_sems": dma((2, 4, CHUNKS)),
        "fw_sems": dma((2, 4, CHUNKS)),
        "pair_sems": dma((2, CHUNKS)),
        "rs_sems": dma((2, 4, CHUNKS)),
        "gz_sems": dma((2, 2, CHUNKS)),
        "fs_sems": dma((2, PLANE)),
        "fp_sems": dma((2, PLANE)),
    }
    names = ["counts_h", "scales_h", "codes_h", "tok_h", "cot_h", "proj", "tg", "out"] + list(scratch)
    shapes = [(local_tokens, key_width), (local_tokens, width), (most, tile, tile)]
    results = pl.pallas_call(
        functools.partial(kernel, names, owners, slots, 1.0 / math.sqrt(total_tokens)),
        in_specs=[hbm] * 5,
        out_specs=[vmem, vmem, vmem],
        out_shape=[pltpu.VMEM(shape, BF16) for shape in shapes],
        scratch_shapes=list(scratch.values()),
        compiler_params=pltpu.CompilerParams(
            collective_id=0, has_side_effects=True, vmem_limit_bytes=44 * 1024 * 1024
        ),
    )(*[
        pltpu.with_memory_space_constraint(v, pltpu.HBM)
        for v in (counts, scales, block_codes, tokens, cotangent)
    ])
    return tuple(pl.pallas_call(
        store_kernel,
        in_specs=[vmem] * 3,
        out_specs=[hbm] * 3,
        out_shape=[pltpu.HBM(shape, BF16) for shape in shapes],
        scratch_shapes=[dma((3,))],
    )(*[pltpu.with_memory_space_constraint(v, pltpu.VMEM) for v in results]))


def solution(mesh):
    return jax.shard_map(
        body,
        mesh=mesh,
        in_specs=(
            P(("dp", "fsdp"), None),
            P("fsdp", None, None),
            P("fsdp"),
            P(),
            P(("dp", "fsdp"), None),
        ),
        out_specs=(P(("dp", "fsdp"), None), P(("dp", "fsdp"), None), P("fsdp", None, None)),
        check_vma=False,
    )
```

```python
import functools
import math
import types

import jax
import jax.numpy as jnp
from jax import lax
from jax.experimental import pallas as pl
from jax.experimental.pallas import tpu as pltpu
from jax.sharding import PartitionSpec as P

MESH = pl.DeviceIdType.MESH
F32 = jnp.float32
BF16 = jnp.bfloat16

PLANE = 4
CORES = 2
GROUP = PLANE * CORES
CHUNKS = 4
SHARED = (2, 3)


def kernel(names, owners, slots, scale, *refs):
    r = types.SimpleNamespace(**dict(zip(names, refs)))
    planes = owners // PLANE
    h = lax.axis_index("dp")
    me = lax.axis_index("fsdp")
    z, c = me // PLANE, me % PLANE
    y, x = c // 2, c % 2
    oy, ox = 1 - y, 1 - x
    most, tile = r.codes_v.shape[0], r.codes_v.shape[1]
    span = r.own_v.shape[1]
    part = span // 2
    places = CHUNKS * span
    blocks = places * GROUP
    period = GROUP * slots
    chunk_blocks = span * GROUP
    plane_most = PLANE * most
    width = r.tok_v.shape[2]
    first, last = pl.ds(0, part), pl.ds(part, span - part)

    x_dev = (h, z * PLANE + 2 * y + ox)
    y_dev = (h, z * PLANE + 2 * oy + x)
    d_dev = (h, z * PLANE + 2 * oy + ox)
    partner = (1 - h, me)
    shared = SHARED if planes % 4 == 0 and part % 2 == 0 else ()
    pair_dev = (h, (z + 1 - 2 * (z % 2)) * PLANE + c)

    def z_dev(d):
        return (h, ((z + 1 - 2 * d + planes) % planes) * PLANE + c)

    def remote(src, dst, send, recv, device):
        return pltpu.make_async_remote_copy(
            src_ref=src, dst_ref=dst, send_sem=send, recv_sem=recv, device_id=device, device_id_type=MESH
        )

    ends = []

    def guarded(conditions, act):
        if conditions:
            pl.when(conditions[0])(lambda: guarded(conditions[1:], act))
        else:
            act()

    def go(copy, when=()):
        guarded(when, copy.start)
        ends.append(lambda: guarded(when, copy.wait_send))
        return copy

    local = [
        pltpu.make_async_copy(r.counts_h, r.counts_s, r.in_sems.at[0]),
        pltpu.make_async_copy(r.scales_h, r.scales_s, r.in_sems.at[1]),
        pltpu.make_async_copy(r.codes_h, r.codes_v, r.in_sems.at[2]),
        pltpu.make_async_copy(r.cot_h, r.cot_v, r.in_sems.at[3]),
    ]
    tok_in = [
        pltpu.make_async_copy(
            r.tok_h.at[:, pl.ds(k * width, width)], r.tok_v.at[k], r.tok_sems.at[k]
        )
        for k in range(CHUNKS)
    ]
    for copy in local + tok_in:
        copy.start()

    barrier = pltpu.get_barrier_semaphore()
    for peer in (x_dev, y_dev, d_dev, partner):
        pl.semaphore_signal(barrier, inc=1, device_id=peer, device_id_type=MESH)
    has_up, has_down = z < planes - 1, z > 0

    @pl.when(has_up)
    def _():
        pl.semaphore_signal(barrier, inc=1, device_id=z_dev(0), device_id_type=MESH)

    @pl.when(has_down)
    def _():
        pl.semaphore_signal(barrier, inc=1, device_id=z_dev(1), device_id_type=MESH)

    for copy in local[:3]:
        copy.wait()
    pl.semaphore_wait(barrier, 4 + jnp.where(has_up, 1, 0) + jnp.where(has_down, 1, 0))

    base, run = 0, [0] * PLANE
    for d in range(owners):
        count = r.counts_s[d]
        base = base + jnp.where(d < z * PLANE, count, 0)
        run[d % PLANE] = run[d % PLANE] + jnp.where(d // PLANE == z, count, 0)
    starts = [base]
    for i in range(PLANE):
        starts.append(starts[-1] + run[i])
    plane_end = starts[PLANE]

    def pick(values, index):
        total = values[0]
        for i in range(1, len(values)):
            total = jnp.where(index == i, values[i], total)
        return total

    my_off = pick(starts[:PLANE], c)
    my_count = pick(run, c)

    p = (2 * z) // planes

    def far_chunk(j):
        return (j + (CHUNKS // 2) * (1 - p)) % CHUNKS

    def near_chunk(j):
        return (j + (CHUNKS // 2) * p) % CHUNKS

    behind = (z, planes - 1 - z)

    def ahead(d, q):
        return q if d == 0 else CHUNKS - 1 - q

    def w_has_recv(d, q):
        return (ahead(d, q) * chunk_blocks < behind[d] * plane_most,)

    def w_has_send(d, q):
        v = behind[d]
        return (v < planes - 1, ahead(d, q) * chunk_blocks < (v + 1) * plane_most)

    def g_has_recv(d, q):
        v = behind[d]
        return (v > 0, ahead(d, CHUNKS - 1 - q) * chunk_blocks < (planes - v) * plane_most)

    def g_has_send(d, q):
        return (ahead(d, CHUNKS - 1 - q) * chunk_blocks < (planes - 1 - behind[d]) * plane_most,)

    def place_block(q, i):
        return (q * span + i) * GROUP + h * PLANE + c

    mates = [(y, x), (y, ox), (oy, x), (oy, ox)]
    mate_devs = [None, x_dev, y_dev, d_dev]

    def scatter():
        for k, (ty, tx) in enumerate(mates):
            target = 2 * ty + tx
            for s in range(slots):
                t = lax.rem(s * GROUP + h * PLANE + target - my_off + blocks, period)
                t = jnp.minimum(t, most - 1)
                block = (r.codes_v[t].astype(F32) * r.scales_s[t]).astype(BF16)
                if k == 0:
                    r.sc_recv[c, s] = block
                else:
                    r.sc_send[k, s] = block
        for k in range(1, PLANE):
            go(scatter_copy(k))

    def scatter_copy(k):
        return remote(r.sc_send.at[k], r.sc_recv.at[c], r.sc_sems.at[0, k], r.sc_sems.at[1, k], mate_devs[k])

    def gather_own():
        for k in range(1, PLANE):
            scatter_copy(k).wait_recv()
        for i in range(PLANE):
            r.sc_loc[i * slots : (i + 1) * slots] = r.sc_recv[i]
        for q in range(CHUNKS):
            for i in range(span):
                b = place_block(q, i)
                owner = 0
                for e in starts[1:PLANE]:
                    owner = owner + jnp.where(b >= e, 1, 0)
                r.own_v[q, i] = r.sc_loc[owner * slots + (q * span + i) % slots]

    def w_task(d, q, when):
        copy = remote(r.w_send.at[d, q], r.w_recv.at[d, q], r.wz_sems.at[0, d, q], r.wz_sems.at[1, d, q], z_dev(d))

        guarded(when + w_has_recv(d, q), copy.wait_recv)

        def merge():
            for i in range(span):
                b = place_block(q, i)
                other = b < base if d == 0 else b >= plane_end
                r.w_send[d, q, i] = jnp.where(other, r.w_recv[d, q, i], r.own_v[q, i])

        sends = when + w_has_send(d, q)
        guarded(sends, merge)
        go(copy, sends)

    def line_order(d, j):
        return (j + CHUNKS // 2) % CHUNKS if d == 0 else j

    def w_primary(j):
        for d in range(2):
            w_task(d, line_order(d, (j + CHUNKS // 2) % CHUNKS), (behind[d] == 0,))
            w_task(d, line_order(d, j), (p == d, behind[d] > 0))

    def w_middle(j):
        for d in range(2):
            w_task(d, line_order(d, j), (p == 1 - d, behind[d] < planes - 1))

    def w_end(j):
        for d in range(2):
            w_task(d, line_order(d, j), (behind[d] == planes - 1,))

    def push(place, k, j):
        return remote(place, place, r.fw_sems.at[0, k, j], r.fw_sems.at[1, k, j], partner)

    def gather_copy(place, k, j, device):
        return remote(place, place, r.ag_sems.at[0, k, j], r.ag_sems.at[1, k, j], device)

    def w_final(j):
        q = near_chunk(j)
        w_end(j)
        for i in range(span):
            b = place_block(q, i)
            r.w_all[h, q, y, x, i] = jnp.where(
                b < base, r.w_recv[0, q, i], jnp.where(b >= plane_end, r.w_recv[1, q, i], r.own_v[q, i])
            )
        place = r.w_all.at[h, q, y, x, gathered(j)]
        go(gather_copy(place, 0, j, x_dev))
        go(gather_copy(place, 1, j, y_dev))
        go(push(r.w_all.at[h, q, y, x], 0, j))

    def gathered(j, half=None, other=False):
        start, size = 0, span
        if j in shared:
            size = part
            start = ((1 - z % 2) if other else z % 2) * part
        if half is not None:
            size = size // 2
            start = start + half * size
        return pl.ds(start, size)

    def w_forward(j):
        q = near_chunk(j)
        for k, (ty, tx) in ((1, (y, ox)), (2, (oy, x))):
            source, device = ((x_dev, y_dev), (y_dev, x_dev))[k - 1]
            place = r.w_all.at[h, q, ty, tx, gathered(j)]
            gather_copy(place, k - 1, j, source).wait_recv()
            go(gather_copy(r.w_all.at[h, q, ty, tx, gathered(j, k - 1)], k + 1, j, device))
            if j in shared:
                go(gather_copy(place, 3 + k, j, pair_dev))
            else:
                go(push(place, k, j))

    def w_diagonal(j):
        q = near_chunk(j)
        gather_copy(r.w_all.at[h, q, oy, ox, gathered(j, 0)], 2, j, y_dev).wait_recv()
        gather_copy(r.w_all.at[h, q, oy, ox, gathered(j, 1)], 3, j, x_dev).wait_recv()
        place = r.w_all.at[h, q, oy, ox, gathered(j)]
        if j in shared:
            go(gather_copy(place, 6, j, pair_dev))
        else:
            go(push(place, 3, j))

    def w_paired(j):
        q = near_chunk(j)
        if j in shared:
            for k in range(1, PLANE):
                ty, tx = mates[k]
                gather_copy(r.w_all.at[h, q, ty, tx, gathered(j, other=True)], 3 + k, j, pair_dev).wait_recv()
                go(push(r.w_all.at[h, q, ty, tx], k, j))

    depth = r.w_mat.shape[0]
    row_tiles = depth // tile

    def products(j):
        q = near_chunk(j)
        for k, (ty, tx) in enumerate(mates):
            push(r.w_all.at[1 - h, q, ty, tx], k, j).wait_recv()
        for rr in range(row_tiles):
            for cc in range(PLANE):
                r.w_mat[rr * tile : (rr + 1) * tile, cc * tile : (cc + 1) * tile] = r.w_all[
                    rr % CORES, q, cc // 2, cc % 2, rr // CORES
                ]
        weight = r.w_mat[...]
        term = jnp.dot(r.tok_v[q], weight, preferred_element_type=F32)
        if j == 0:
            r.acc[...] = term
        elif j < CHUNKS - 1:
            r.acc[...] += term
        else:
            r.proj[...] = (r.acc[...] + term).astype(BF16)
        r.tg[:, pl.ds(pl.multiple_of(q * depth, depth), depth)] = lax.dot_general(
            r.cot_v[...], weight, (((1,), (1,)), ((), ())), preferred_element_type=F32
        ).astype(BF16)

    steps = 2
    sub = depth // steps

    def pair_copy(j):
        q = far_chunk(j)
        return remote(r.g_terms.at[1 - h, q], r.g_pair.at[q], r.pair_sems.at[0, j], r.pair_sems.at[1, j], partner)

    def terms(j):
        q = far_chunk(j)
        for g in range(steps):
            value = lax.dot_general(
                r.tok_v[q, :, g * sub : (g + 1) * sub], r.cot_v[...], (((0,), (0,)), ((), ())),
                preferred_element_type=F32,
            )
            value = (value * scale).astype(BF16)
            for rr in range(sub // tile):
                row = g * (sub // tile) + rr
                for cc in range(PLANE):
                    r.g_terms[row % CORES, q, cc // 2, cc % 2, row // CORES] = value[
                        rr * tile : (rr + 1) * tile, cc * tile : (cc + 1) * tile
                    ]
        go(pair_copy(j))

    def pair_sum(j):
        q = far_chunk(j)
        pair_copy(j).wait_recv()

        for a in range(2):
            for b in range(2):
                r.g_sum[q, a, b] = (r.g_terms[h, q, a, b].astype(F32) + r.g_pair[q, a, b].astype(F32)).astype(BF16)

    def rs_one(j):
        q = far_chunk(j)
        return [
            remote(r.g_sum.at[q, oy, :, first], r.r1a.at[q], r.rs_sems.at[0, 0, j], r.rs_sems.at[1, 0, j], y_dev),
            remote(r.g_sum.at[q, :, ox, last], r.r1b.at[q], r.rs_sems.at[0, 1, j], r.rs_sems.at[1, 1, j], x_dev),
        ]

    def rs_two(j):
        q = far_chunk(j)
        return [
            remote(r.s2a.at[q], r.r2a.at[q], r.rs_sems.at[0, 2, j], r.rs_sems.at[1, 2, j], x_dev),
            remote(r.s2b.at[q], r.r2b.at[q], r.rs_sems.at[0, 3, j], r.rs_sems.at[1, 3, j], y_dev),
        ]

    def reduce_one(j):
        for copy in rs_one(j):
            go(copy)

    def reduce_two(j):
        q = far_chunk(j)
        one, two = rs_one(j), rs_two(j)
        one[0].wait_recv()
        r.s2a[q] = (r.g_sum[q, y, ox, first].astype(F32) + r.r1a[q, ox].astype(F32)).astype(BF16)
        go(two[0])
        one[1].wait_recv()
        r.s2b[q] = (r.g_sum[q, oy, x, last].astype(F32) + r.r1b[q, oy].astype(F32)).astype(BF16)
        go(two[1])

    def plane_sum(j):
        q = far_chunk(j)
        two = rs_two(j)
        two[0].wait_recv()
        r.g_plane[q, first] = (
            r.g_sum[q, y, x, first].astype(F32) + r.r1a[q, x].astype(F32) + r.r2a[q].astype(F32)
        )
        two[1].wait_recv()
        r.g_plane[q, last] = (
            r.g_sum[q, y, x, last].astype(F32) + r.r1b[q, y].astype(F32) + r.r2b[q].astype(F32)
        )

    def behind_sum(d, q):
        return jnp.where(behind[d] > 0, r.gz_recv[d, q].astype(F32), 0.0)

    def g_task(d, q, when):
        copy = remote(r.gz_send.at[d, q], r.gz_recv.at[d, q], r.gz_sems.at[0, d, q], r.gz_sems.at[1, d, q], z_dev(d))

        guarded(when + g_has_recv(d, q), copy.wait_recv)

        def add():
            r.gz_send[d, q] = (r.g_plane[q] + behind_sum(d, q)).astype(BF16)

        sends = when + g_has_send(d, q)
        guarded(sends, add)
        go(copy, sends)

    def g_first(j):
        for d in range(2):
            g_task(d, line_order(d, j), (behind[d] == 0,))

    def g_next(j):
        for d in range(2):
            g_task(d, line_order(d, j), (p == d, behind[d] > 0))

    def g_middle(j):
        for d in range(2):
            g_task(d, line_order(d, j), (p == 1 - d, behind[d] < planes - 1))

    def g_final(j):
        for d in range(2):
            g_task(d, line_order(d, j), (behind[d] == planes - 1,))
        q = near_chunk(j)
        r.g_full[pl.ds(q * span, span)] = (r.g_plane[q] + behind_sum(0, q) + behind_sum(1, q)).astype(BF16)

    def owner_copy(k):
        return remote(r.fs_send.at[k], r.fs_all.at[h, c], r.fs_sems.at[0, k], r.fs_sems.at[1, k], mate_devs[k])

    def give(k):
        ty, tx = mates[k]
        place = r.fs_all.at[h, 2 * ty + tx]
        return remote(place, place, r.fp_sems.at[0, k], r.fp_sems.at[1, k], partner)

    def to_owners():
        for k in (3, 1, 2, 0):
            ty, tx = mates[k]
            off = pick(starts[:PLANE], 2 * ty + tx)
            for s in range(slots):
                t = lax.rem(s * GROUP + h * PLANE + c - off + blocks, period)
                m = jnp.minimum(lax.div(off + t, GROUP), places - 1)
                block = r.g_full[m]
                if k == 0:
                    r.fs_all[h, c, s] = block
                else:
                    r.fs_send[k, s] = block
        for k in (3, 1, 2):
            go(owner_copy(k))
        go(give(0))

    def share_owned():
        for k in (1, 2, 3):
            owner_copy(k).wait_recv()
            go(give(k))

    def finish():
        for k in range(PLANE):
            ty, tx = mates[k]
            place = r.fs_all.at[1 - h, 2 * ty + tx]
            remote(place, place, r.fp_sems.at[0, k], r.fp_sems.at[1, k], partner).wait_recv()
        for k in range(CORES * PLANE):
            r.fs_loc[k * slots : (k + 1) * slots] = r.fs_all[k // PLANE, k % PLANE]
        for j in range(most):
            b = my_off + j
            block = r.fs_loc[lax.rem(b, GROUP) * slots + lax.rem(lax.div(b, GROUP), slots)]
            r.out[j] = jnp.where(j < my_count, block, jnp.zeros_like(block))

    scatter()
    local[3].wait()
    for copy in tok_in:
        copy.wait()
    for j in range(CHUNKS):
        terms(j)
    pair_sum(0)
    reduce_one(0)
    pair_sum(1)
    reduce_one(1)
    gather_own()
    w_primary(0)
    w_primary(1)
    pair_sum(2)
    pair_sum(3)
    reduce_two(0)
    reduce_one(2)
    w_primary(2)
    w_middle(0)
    reduce_two(1)
    reduce_one(3)
    w_primary(3)
    plane_sum(0)
    g_first(0)
    w_middle(1)
    reduce_two(2)
    w_middle(2)
    plane_sum(1)
    g_first(1)
    g_next(0)
    w_middle(3)
    reduce_two(3)
    w_final(0)
    w_final(1)
    plane_sum(2)
    g_first(2)
    g_next(1)
    g_middle(0)
    plane_sum(3)
    g_first(3)
    w_final(2)
    w_final(3)
    w_forward(0)
    g_next(2)
    g_middle(1)
    w_forward(1)
    g_next(3)
    w_forward(2)
    w_forward(3)
    w_diagonal(0)
    g_middle(2)
    w_diagonal(1)
    g_middle(3)
    g_final(0)
    g_final(1)
    g_final(2)
    g_final(3)
    to_owners()
    w_diagonal(2)
    w_paired(0)
    products(0)
    w_diagonal(3)
    w_paired(1)
    products(1)
    w_paired(2)
    share_owned()
    w_paired(3)
    products(2)
    finish()
    products(3)
    for end in ends:
        end()


def store_kernel(proj, tg, out, proj_h, tg_h, out_h, sems):
    copies = [
        pltpu.make_async_copy(src, dst, sems.at[k])
        for k, (src, dst) in enumerate([(tg, tg_h), (out, out_h), (proj, proj_h)])
    ]
    for copy in copies:
        copy.start()
    for copy in copies:
        copy.wait()


def body(tokens, block_codes, scales, counts, cotangent):
    owners = lax.axis_size("fsdp")
    most, tile = block_codes.shape[0], block_codes.shape[1]
    local_tokens, width = tokens.shape
    key_width = cotangent.shape[1]
    blocks = (width // tile) * (key_width // tile)
    total_tokens = local_tokens * lax.axis_size("dp") * owners
    slots = -(-most // GROUP)
    span = blocks // (GROUP * CHUNKS)
    depth = width // CHUNKS
    assert lax.axis_size("dp") == CORES and owners % PLANE == 0 and key_width == PLANE * tile
    assert span * GROUP * CHUNKS == blocks and span % 2 == 0 and span % slots == 0

    dma = pltpu.SemaphoreType.DMA
    vmem = pl.BlockSpec(memory_space=pltpu.VMEM)
    hbm = pl.BlockSpec(memory_space=pltpu.HBM)

    def held(*shape, kind=BF16):
        return pltpu.VMEM(shape + (tile, tile), kind)

    half, places = span // 2, span * CHUNKS
    scratch = {
        "counts_s": pltpu.SMEM(counts.shape, jnp.int32),
        "scales_s": pltpu.SMEM(scales.shape, F32),
        "codes_v": pltpu.VMEM(block_codes.shape, BF16),
        "cot_v": pltpu.VMEM(cotangent.shape, BF16),
        "tok_v": pltpu.VMEM((CHUNKS, local_tokens, depth), BF16),
        "sc_send": held(PLANE, slots),
        "sc_recv": held(PLANE, slots),
        "sc_loc": held(PLANE * slots),
        "fs_loc": held(CORES * PLANE * slots),
        "own_v": held(CHUNKS, span),
        "w_send": held(2, CHUNKS, span),
        "w_recv": held(2, CHUNKS, span),
        "w_all": held(CORES, CHUNKS, 2, 2, span),
        "w_mat": pltpu.VMEM((depth, key_width), BF16),
        "acc": pltpu.VMEM((local_tokens, key_width), F32),
        "g_terms": held(CORES, CHUNKS, 2, 2, span),
        "g_pair": held(CHUNKS, 2, 2, span),
        "g_sum": held(CHUNKS, 2, 2, span),
        "r1a": held(CHUNKS, 2, half),
        "r1b": held(CHUNKS, 2, half),
        "s2a": held(CHUNKS, half),
        "s2b": held(CHUNKS, half),
        "r2a": held(CHUNKS, half),
        "r2b": held(CHUNKS, half),
        "g_plane": held(CHUNKS, span, kind=F32),
        "gz_send": held(2, CHUNKS, span),
        "gz_recv": held(2, CHUNKS, span),
        "g_full": held(places),
        "fs_send": held(PLANE, slots),
        "fs_all": held(CORES, PLANE, slots),
        "in_sems": dma((4,)),
        "tok_sems": dma((CHUNKS,)),
        "sc_sems": dma((2, PLANE)),
        "wz_sems": dma((2, 2, CHUNKS)),
        "ag_sems": dma((2, 7, CHUNKS)),
        "fw_sems": dma((2, 4, CHUNKS)),
        "pair_sems": dma((2, CHUNKS)),
        "rs_sems": dma((2, 4, CHUNKS)),
        "gz_sems": dma((2, 2, CHUNKS)),
        "fs_sems": dma((2, PLANE)),
        "fp_sems": dma((2, PLANE)),
    }
    names = ["counts_h", "scales_h", "codes_h", "tok_h", "cot_h", "proj", "tg", "out"] + list(scratch)
    shapes = [(local_tokens, key_width), (local_tokens, width), (most, tile, tile)]
    results = pl.pallas_call(
        functools.partial(kernel, names, owners, slots, 1.0 / math.sqrt(total_tokens)),
        in_specs=[hbm] * 5,
        out_specs=[vmem, vmem, vmem],
        out_shape=[pltpu.VMEM(shape, BF16) for shape in shapes],
        scratch_shapes=list(scratch.values()),
        compiler_params=pltpu.CompilerParams(
            collective_id=0, has_side_effects=True, vmem_limit_bytes=44 * 1024 * 1024
        ),
    )(*[
        pltpu.with_memory_space_constraint(v, pltpu.HBM)
        for v in (counts, scales, block_codes, tokens, cotangent)
    ])
    return tuple(pl.pallas_call(
        store_kernel,
        in_specs=[vmem] * 3,
        out_specs=[hbm] * 3,
        out_shape=[pltpu.HBM(shape, BF16) for shape in shapes],
        scratch_shapes=[dma((3,))],
    )(*[pltpu.with_memory_space_constraint(v, pltpu.VMEM) for v in results]))


def solution(mesh):
    return jax.shard_map(
        body,
        mesh=mesh,
        in_specs=(
            P(("dp", "fsdp"), None),
            P("fsdp", None, None),
            P("fsdp"),
            P(),
            P(("dp", "fsdp"), None),
        ),
        out_specs=(P(("dp", "fsdp"), None), P(("dp", "fsdp"), None), P("fsdp", None, None)),
        check_vma=False,
    )
```

```python
import functools
import math
import types

import jax
import jax.numpy as jnp
from jax import lax
from jax.experimental import pallas as pl
from jax.experimental.pallas import tpu as pltpu
from jax.sharding import PartitionSpec as P

MESH = pl.DeviceIdType.MESH
F32 = jnp.float32
BF16 = jnp.bfloat16

PLANE = 4
CORES = 2
GROUP = PLANE * CORES
CHUNKS = 4
SHARED = (2, 3)


def kernel(names, owners, slots, scale, *refs):
    r = types.SimpleNamespace(**dict(zip(names, refs)))
    planes = owners // PLANE
    h = lax.axis_index("dp")
    me = lax.axis_index("fsdp")
    z, c = me // PLANE, me % PLANE
    y, x = c // 2, c % 2
    oy, ox = 1 - y, 1 - x
    most, tile = r.codes_v.shape[0], r.codes_v.shape[1]
    span = r.own_v.shape[1]
    part = span // 2
    places = CHUNKS * span
    blocks = places * GROUP
    period = GROUP * slots
    chunk_blocks = span * GROUP
    plane_most = PLANE * most
    width = r.tok_v.shape[2]
    first, last = pl.ds(0, part), pl.ds(part, span - part)

    x_dev = (h, z * PLANE + 2 * y + ox)
    y_dev = (h, z * PLANE + 2 * oy + x)
    d_dev = (h, z * PLANE + 2 * oy + ox)
    partner = (1 - h, me)
    shared = SHARED if planes % 4 == 0 and part % 2 == 0 else ()
    pair_dev = (h, (z + 1 - 2 * (z % 2)) * PLANE + c)

    def z_dev(d):
        return (h, ((z + 1 - 2 * d + planes) % planes) * PLANE + c)

    def remote(src, dst, send, recv, device):
        return pltpu.make_async_remote_copy(
            src_ref=src, dst_ref=dst, send_sem=send, recv_sem=recv, device_id=device, device_id_type=MESH
        )

    ends = []

    def guarded(conditions, act):
        if conditions:
            pl.when(conditions[0])(lambda: guarded(conditions[1:], act))
        else:
            act()

    def go(copy, when=()):
        guarded(when, copy.start)
        ends.append(lambda: guarded(when, copy.wait_send))
        return copy

    local = [
        pltpu.make_async_copy(r.counts_h, r.counts_s, r.in_sems.at[0]),
        pltpu.make_async_copy(r.scales_h, r.scales_s, r.in_sems.at[1]),
        pltpu.make_async_copy(r.codes_h, r.codes_v, r.in_sems.at[2]),
        pltpu.make_async_copy(r.cot_h, r.cot_v, r.in_sems.at[3]),
    ]
    tok_in = [
        pltpu.make_async_copy(
            r.tok_h.at[:, pl.ds(k * width, width)], r.tok_v.at[k], r.tok_sems.at[k]
        )
        for k in range(CHUNKS)
    ]
    for copy in local + tok_in:
        copy.start()

    barrier = pltpu.get_barrier_semaphore()
    for peer in (x_dev, y_dev, d_dev, partner):
        pl.semaphore_signal(barrier, inc=1, device_id=peer, device_id_type=MESH)
    has_up, has_down = z < planes - 1, z > 0

    @pl.when(has_up)
    def _():
        pl.semaphore_signal(barrier, inc=1, device_id=z_dev(0), device_id_type=MESH)

    @pl.when(has_down)
    def _():
        pl.semaphore_signal(barrier, inc=1, device_id=z_dev(1), device_id_type=MESH)

    for copy in local[:3]:
        copy.wait()
    pl.semaphore_wait(barrier, 4 + jnp.where(has_up, 1, 0) + jnp.where(has_down, 1, 0))

    base, run = 0, [0] * PLANE
    for d in range(owners):
        count = r.counts_s[d]
        base = base + jnp.where(d < z * PLANE, count, 0)
        run[d % PLANE] = run[d % PLANE] + jnp.where(d // PLANE == z, count, 0)
    starts = [base]
    for i in range(PLANE):
        starts.append(starts[-1] + run[i])
    plane_end = starts[PLANE]

    def pick(values, index):
        total = values[0]
        for i in range(1, len(values)):
            total = jnp.where(index == i, values[i], total)
        return total

    my_off = pick(starts[:PLANE], c)
    my_count = pick(run, c)

    p = (2 * z) // planes

    def far_chunk(j):
        return (j + (CHUNKS // 2) * (1 - p)) % CHUNKS

    def near_chunk(j):
        return (j + (CHUNKS // 2) * p) % CHUNKS

    behind = (z, planes - 1 - z)

    def ahead(d, q):
        return q if d == 0 else CHUNKS - 1 - q

    def w_has_recv(d, q):
        return (ahead(d, q) * chunk_blocks < behind[d] * plane_most,)

    def w_has_send(d, q):
        v = behind[d]
        return (v < planes - 1, ahead(d, q) * chunk_blocks < (v + 1) * plane_most)

    def g_has_recv(d, q):
        v = behind[d]
        return (v > 0, ahead(d, CHUNKS - 1 - q) * chunk_blocks < (planes - v) * plane_most)

    def g_has_send(d, q):
        return (ahead(d, CHUNKS - 1 - q) * chunk_blocks < (planes - 1 - behind[d]) * plane_most,)

    def place_block(q, i):
        return (q * span + i) * GROUP + h * PLANE + c

    mates = [(y, x), (y, ox), (oy, x), (oy, ox)]
    mate_devs = [None, x_dev, y_dev, d_dev]

    def scatter():
        for k, (ty, tx) in enumerate(mates):
            target = 2 * ty + tx
            for s in range(slots):
                t = lax.rem(s * GROUP + h * PLANE + target - my_off + blocks, period)
                t = jnp.minimum(t, most - 1)
                block = (r.codes_v[t].astype(F32) * r.scales_s[t]).astype(BF16)
                if k == 0:
                    r.sc_recv[c, s] = block
                else:
                    r.sc_send[k, s] = block
        for k in range(1, PLANE):
            go(scatter_copy(k))

    def scatter_copy(k):
        return remote(r.sc_send.at[k], r.sc_recv.at[c], r.sc_sems.at[0, k], r.sc_sems.at[1, k], mate_devs[k])

    def gather_own():
        for k in range(1, PLANE):
            scatter_copy(k).wait_recv()
        for i in range(PLANE):
            r.sc_loc[i * slots : (i + 1) * slots] = r.sc_recv[i]
        for q in range(CHUNKS):
            for i in range(span):
                b = place_block(q, i)
                owner = 0
                for e in starts[1:PLANE]:
                    owner = owner + jnp.where(b >= e, 1, 0)
                r.own_v[q, i] = r.sc_loc[owner * slots + (q * span + i) % slots]

    def w_task(d, q, when):
        copy = remote(r.w_send.at[d, q], r.w_recv.at[d, q], r.wz_sems.at[0, d, q], r.wz_sems.at[1, d, q], z_dev(d))

        guarded(when + w_has_recv(d, q), copy.wait_recv)

        def merge():
            for i in range(span):
                b = place_block(q, i)
                other = b < base if d == 0 else b >= plane_end
                r.w_send[d, q, i] = jnp.where(other, r.w_recv[d, q, i], r.own_v[q, i])

        sends = when + w_has_send(d, q)
        guarded(sends, merge)
        go(copy, sends)

    def line_order(d, j):
        return (j + CHUNKS // 2) % CHUNKS if d == 0 else j

    def w_primary(j):
        for d in range(2):
            w_task(d, line_order(d, (j + CHUNKS // 2) % CHUNKS), (behind[d] == 0,))
            w_task(d, line_order(d, j), (p == d, behind[d] > 0))

    def w_middle(j):
        for d in range(2):
            w_task(d, line_order(d, j), (p == 1 - d, behind[d] < planes - 1))

    def w_end(j):
        for d in range(2):
            w_task(d, line_order(d, j), (behind[d] == planes - 1,))

    def push(place, k, j):
        return remote(place, place, r.fw_sems.at[0, k, j], r.fw_sems.at[1, k, j], partner)

    def gather_copy(place, k, j, device):
        return remote(place, place, r.ag_sems.at[0, k, j], r.ag_sems.at[1, k, j], device)

    def w_final(j):
        q = near_chunk(j)
        w_end(j)
        for i in range(span):
            b = place_block(q, i)
            r.w_all[h, q, y, x, i] = jnp.where(
                b < base, r.w_recv[0, q, i], jnp.where(b >= plane_end, r.w_recv[1, q, i], r.own_v[q, i])
            )
        place = r.w_all.at[h, q, y, x, gathered(j)]
        go(gather_copy(place, 0, j, x_dev))
        go(gather_copy(place, 1, j, y_dev))
        go(push(r.w_all.at[h, q, y, x], 0, j))

    def gathered(j, half=None, other=False):
        start, size = 0, span
        if j in shared:
            size = part
            start = ((1 - z % 2) if other else z % 2) * part
        if half is not None:
            size = size // 2
            start = start + half * size
        return pl.ds(start, size)

    def w_forward(j):
        q = near_chunk(j)
        for k, (ty, tx) in ((1, (y, ox)), (2, (oy, x))):
            source, device = ((x_dev, y_dev), (y_dev, x_dev))[k - 1]
            place = r.w_all.at[h, q, ty, tx, gathered(j)]
            gather_copy(place, k - 1, j, source).wait_recv()
            go(gather_copy(r.w_all.at[h, q, ty, tx, gathered(j, k - 1)], k + 1, j, device))
            if j in shared:
                go(gather_copy(place, 3 + k, j, pair_dev))
            go(push(place, k, j))

    def w_diagonal(j):
        q = near_chunk(j)
        gather_copy(r.w_all.at[h, q, oy, ox, gathered(j, 0)], 2, j, y_dev).wait_recv()
        gather_copy(r.w_all.at[h, q, oy, ox, gathered(j, 1)], 3, j, x_dev).wait_recv()
        place = r.w_all.at[h, q, oy, ox, gathered(j)]
        if j in shared:
            go(gather_copy(place, 6, j, pair_dev))
        go(push(place, 3, j))

    def w_paired(j):
        q = near_chunk(j)
        if j in shared:
            for k in range(1, PLANE):
                ty, tx = mates[k]
                place = r.w_all.at[h, q, ty, tx, gathered(j, other=True)]
                gather_copy(place, 3 + k, j, pair_dev).wait_recv()
                go(push(place, 3 + k, j))

    depth = r.w_mat.shape[0]
    row_tiles = depth // tile

    def products(j):
        q = near_chunk(j)
        push(r.w_all.at[1 - h, q, y, x], 0, j).wait_recv()
        for k in range(1, PLANE):
            ty, tx = mates[k]
            push(r.w_all.at[1 - h, q, ty, tx, gathered(j)], k, j).wait_recv()
            if j in shared:
                push(r.w_all.at[1 - h, q, ty, tx, gathered(j, other=True)], 3 + k, j).wait_recv()
        for rr in range(row_tiles):
            for cc in range(PLANE):
                r.w_mat[rr * tile : (rr + 1) * tile, cc * tile : (cc + 1) * tile] = r.w_all[
                    rr % CORES, q, cc // 2, cc % 2, rr // CORES
                ]
        if j == CHUNKS - 1:
            return
        weight = r.w_mat[...]
        term = jnp.dot(r.tok_v[q], weight, preferred_element_type=F32)
        if j == 0:
            r.acc[...] = term
        else:
            r.acc[...] += term
        r.tg[:, pl.ds(pl.multiple_of(q * depth, depth), depth)] = lax.dot_general(
            r.cot_v[...], weight, (((1,), (1,)), ((), ())), preferred_element_type=F32
        ).astype(BF16)

    def keep_last():
        r.tok_last[...] = r.tok_v[near_chunk(CHUNKS - 1)]
        r.cot_last[...] = r.cot_v[...]

    steps = 2
    sub = depth // steps

    def pair_copy(j):
        q = far_chunk(j)
        return remote(r.g_terms.at[1 - h, q], r.g_pair.at[q], r.pair_sems.at[0, j], r.pair_sems.at[1, j], partner)

    def terms(j):
        q = far_chunk(j)
        for g in range(steps):
            value = lax.dot_general(
                r.tok_v[q, :, g * sub : (g + 1) * sub], r.cot_v[...], (((0,), (0,)), ((), ())),
                preferred_element_type=F32,
            )
            value = (value * scale).astype(BF16)
            for rr in range(sub // tile):
                row = g * (sub // tile) + rr
                for cc in range(PLANE):
                    r.g_terms[row % CORES, q, cc // 2, cc % 2, row // CORES] = value[
                        rr * tile : (rr + 1) * tile, cc * tile : (cc + 1) * tile
                    ]
        go(pair_copy(j))

    def pair_sum(j):
        q = far_chunk(j)
        pair_copy(j).wait_recv()

        for a in range(2):
            for b in range(2):
                r.g_sum[q, a, b] = (r.g_terms[h, q, a, b].astype(F32) + r.g_pair[q, a, b].astype(F32)).astype(BF16)

    def rs_one(j):
        q = far_chunk(j)
        return [
            remote(r.g_sum.at[q, oy, :, first], r.r1a.at[q], r.rs_sems.at[0, 0, j], r.rs_sems.at[1, 0, j], y_dev),
            remote(r.g_sum.at[q, :, ox, last], r.r1b.at[q], r.rs_sems.at[0, 1, j], r.rs_sems.at[1, 1, j], x_dev),
        ]

    def rs_two(j):
        q = far_chunk(j)
        return [
            remote(r.s2a.at[q], r.r2a.at[q], r.rs_sems.at[0, 2, j], r.rs_sems.at[1, 2, j], x_dev),
            remote(r.s2b.at[q], r.r2b.at[q], r.rs_sems.at[0, 3, j], r.rs_sems.at[1, 3, j], y_dev),
        ]

    def reduce_one(j):
        for copy in rs_one(j):
            go(copy)

    def reduce_two(j):
        q = far_chunk(j)
        one, two = rs_one(j), rs_two(j)
        one[0].wait_recv()
        r.s2a[q] = (r.g_sum[q, y, ox, first].astype(F32) + r.r1a[q, ox].astype(F32)).astype(BF16)
        go(two[0])
        one[1].wait_recv()
        r.s2b[q] = (r.g_sum[q, oy, x, last].astype(F32) + r.r1b[q, oy].astype(F32)).astype(BF16)
        go(two[1])

    def plane_sum(j):
        q = far_chunk(j)
        two = rs_two(j)
        two[0].wait_recv()
        r.g_plane[q, first] = (
            r.g_sum[q, y, x, first].astype(F32) + r.r1a[q, x].astype(F32) + r.r2a[q].astype(F32)
        )
        two[1].wait_recv()
        r.g_plane[q, last] = (
            r.g_sum[q, y, x, last].astype(F32) + r.r1b[q, y].astype(F32) + r.r2b[q].astype(F32)
        )

    def behind_sum(d, q):
        return jnp.where(behind[d] > 0, r.gz_recv[d, q].astype(F32), 0.0)

    def g_task(d, q, when):
        copy = remote(r.gz_send.at[d, q], r.gz_recv.at[d, q], r.gz_sems.at[0, d, q], r.gz_sems.at[1, d, q], z_dev(d))

        guarded(when + g_has_recv(d, q), copy.wait_recv)

        def add():
            r.gz_send[d, q] = (r.g_plane[q] + behind_sum(d, q)).astype(BF16)

        sends = when + g_has_send(d, q)
        guarded(sends, add)
        go(copy, sends)

    def g_first(j):
        for d in range(2):
            g_task(d, line_order(d, j), (behind[d] == 0,))

    def g_next(j):
        for d in range(2):
            g_task(d, line_order(d, j), (p == d, behind[d] > 0))

    def g_middle(j):
        for d in range(2):
            g_task(d, line_order(d, j), (p == 1 - d, behind[d] < planes - 1))

    def g_final(j):
        for d in range(2):
            g_task(d, line_order(d, j), (behind[d] == planes - 1,))
        q = near_chunk(j)
        r.g_full[pl.ds(q * span, span)] = (r.g_plane[q] + behind_sum(0, q) + behind_sum(1, q)).astype(BF16)

    def owner_copy(k):
        return remote(r.fs_send.at[k], r.fs_all.at[h, c], r.fs_sems.at[0, k], r.fs_sems.at[1, k], mate_devs[k])

    def give(k):
        ty, tx = mates[k]
        place = r.fs_all.at[h, 2 * ty + tx]
        return remote(place, place, r.fp_sems.at[0, k], r.fp_sems.at[1, k], partner)

    def to_owners():
        for k in (3, 1, 2, 0):
            ty, tx = mates[k]
            off = pick(starts[:PLANE], 2 * ty + tx)
            for s in range(slots):
                t = lax.rem(s * GROUP + h * PLANE + c - off + blocks, period)
                m = jnp.minimum(lax.div(off + t, GROUP), places - 1)
                block = r.g_full[m]
                if k == 0:
                    r.fs_all[h, c, s] = block
                else:
                    r.fs_send[k, s] = block
        for k in (3, 1, 2):
            go(owner_copy(k))
        go(give(0))

    def share_owned():
        for k in (1, 2, 3):
            owner_copy(k).wait_recv()
            go(give(k))

    def finish():
        for k in range(PLANE):
            ty, tx = mates[k]
            place = r.fs_all.at[1 - h, 2 * ty + tx]
            remote(place, place, r.fp_sems.at[0, k], r.fp_sems.at[1, k], partner).wait_recv()
        for k in range(CORES * PLANE):
            r.fs_loc[k * slots : (k + 1) * slots] = r.fs_all[k // PLANE, k % PLANE]
        for j in range(most):
            b = my_off + j
            block = r.fs_loc[lax.rem(b, GROUP) * slots + lax.rem(lax.div(b, GROUP), slots)]
            r.out[j] = jnp.where(j < my_count, block, jnp.zeros_like(block))

    scatter()
    local[3].wait()
    for copy in tok_in:
        copy.wait()
    for j in range(CHUNKS):
        terms(j)
    pair_sum(0)
    reduce_one(0)
    pair_sum(1)
    reduce_one(1)
    pair_sum(2)
    pair_sum(3)
    gather_own()
    w_primary(0)
    w_primary(1)
    reduce_two(0)
    reduce_one(2)
    w_primary(2)
    w_middle(0)
    reduce_two(1)
    reduce_one(3)
    w_primary(3)
    plane_sum(0)
    g_first(0)
    w_middle(1)
    reduce_two(2)
    w_middle(2)
    plane_sum(1)
    g_first(1)
    g_next(0)
    w_middle(3)
    reduce_two(3)
    w_final(0)
    w_final(1)
    plane_sum(2)
    g_first(2)
    g_next(1)
    g_middle(0)
    plane_sum(3)
    g_first(3)
    w_final(2)
    w_final(3)
    keep_last()
    w_forward(0)
    g_next(2)
    g_middle(1)
    w_forward(1)
    g_next(3)
    w_forward(2)
    w_forward(3)
    g_middle(2)
    g_middle(3)
    g_final(0)
    g_final(1)
    g_final(2)
    g_final(3)
    to_owners()
    w_diagonal(0)
    w_diagonal(1)
    w_diagonal(2)
    w_paired(0)
    products(0)
    w_diagonal(3)
    w_paired(1)
    products(1)
    w_paired(2)
    share_owned()
    w_paired(3)
    products(2)
    finish()
    products(3)
    for end in ends:
        end()


def last_kernel(planes, acc, tg, out, w_mat, tok_last, cot_last, proj_h, tg_h, out_h, proj_v, tail_v, sems):
    depth = w_mat.shape[0]
    p = (2 * (lax.axis_index("fsdp") // PLANE)) // planes
    q = (CHUNKS - 1 + (CHUNKS // 2) * p) % CHUNKS

    def columns(chunk):
        return pl.ds(pl.multiple_of(chunk * depth, depth), depth)

    copies = [pltpu.make_async_copy(out, out_h, sems.at[0])]
    for k in range(1, CHUNKS):
        place = columns((q + k) % CHUNKS)
        copies.append(pltpu.make_async_copy(tg.at[:, place], tg_h.at[:, place], sems.at[k]))
    for copy in copies:
        copy.start()
    weight = w_mat[...]
    tail_v[...] = lax.dot_general(
        cot_last[...], weight, (((1,), (1,)), ((), ())), preferred_element_type=F32
    ).astype(BF16)
    copies.append(pltpu.make_async_copy(tail_v, tg_h.at[:, columns(q)], sems.at[CHUNKS]))
    copies[-1].start()
    proj_v[...] = (acc[...] + jnp.dot(tok_last[...], weight, preferred_element_type=F32)).astype(BF16)
    copies.append(pltpu.make_async_copy(proj_v, proj_h, sems.at[CHUNKS + 1]))
    copies[-1].start()
    for copy in copies:
        copy.wait()


def body(tokens, block_codes, scales, counts, cotangent):
    owners = lax.axis_size("fsdp")
    most, tile = block_codes.shape[0], block_codes.shape[1]
    local_tokens, width = tokens.shape
    key_width = cotangent.shape[1]
    blocks = (width // tile) * (key_width // tile)
    total_tokens = local_tokens * lax.axis_size("dp") * owners
    slots = -(-most // GROUP)
    span = blocks // (GROUP * CHUNKS)
    depth = width // CHUNKS
    assert lax.axis_size("dp") == CORES and owners % PLANE == 0 and key_width == PLANE * tile
    assert span * GROUP * CHUNKS == blocks and span % 2 == 0 and span % slots == 0

    dma = pltpu.SemaphoreType.DMA
    vmem = pl.BlockSpec(memory_space=pltpu.VMEM)
    hbm = pl.BlockSpec(memory_space=pltpu.HBM)

    def held(*shape, kind=BF16):
        return pltpu.VMEM(shape + (tile, tile), kind)

    half, places = span // 2, span * CHUNKS
    scratch = {
        "counts_s": pltpu.SMEM(counts.shape, jnp.int32),
        "scales_s": pltpu.SMEM(scales.shape, F32),
        "codes_v": pltpu.VMEM(block_codes.shape, BF16),
        "cot_v": pltpu.VMEM(cotangent.shape, BF16),
        "tok_v": pltpu.VMEM((CHUNKS, local_tokens, depth), BF16),
        "sc_send": held(PLANE, slots),
        "sc_recv": held(PLANE, slots),
        "sc_loc": held(PLANE * slots),
        "fs_loc": held(CORES * PLANE * slots),
        "own_v": held(CHUNKS, span),
        "w_send": held(2, CHUNKS, span),
        "w_recv": held(2, CHUNKS, span),
        "w_all": held(CORES, CHUNKS, 2, 2, span),
        "g_terms": held(CORES, CHUNKS, 2, 2, span),
        "g_pair": held(CHUNKS, 2, 2, span),
        "g_sum": held(CHUNKS, 2, 2, span),
        "r1a": held(CHUNKS, 2, half),
        "r1b": held(CHUNKS, 2, half),
        "s2a": held(CHUNKS, half),
        "s2b": held(CHUNKS, half),
        "r2a": held(CHUNKS, half),
        "r2b": held(CHUNKS, half),
        "g_plane": held(CHUNKS, span, kind=F32),
        "gz_send": held(2, CHUNKS, span),
        "gz_recv": held(2, CHUNKS, span),
        "g_full": held(places),
        "fs_send": held(PLANE, slots),
        "fs_all": held(CORES, PLANE, slots),
        "in_sems": dma((4,)),
        "tok_sems": dma((CHUNKS,)),
        "sc_sems": dma((2, PLANE)),
        "wz_sems": dma((2, 2, CHUNKS)),
        "ag_sems": dma((2, 7, CHUNKS)),
        "fw_sems": dma((2, 7, CHUNKS)),
        "pair_sems": dma((2, CHUNKS)),
        "rs_sems": dma((2, 4, CHUNKS)),
        "gz_sems": dma((2, 2, CHUNKS)),
        "fs_sems": dma((2, PLANE)),
        "fp_sems": dma((2, PLANE)),
    }
    names = ["counts_h", "scales_h", "codes_h", "tok_h", "cot_h", "acc", "tg", "out", "w_mat", "tok_last", "cot_last"] + list(scratch)
    shapes = [(local_tokens, key_width), (local_tokens, width), (most, tile, tile)]
    planes = owners // PLANE
    kept = [pltpu.VMEM(shapes[0], F32)] + [
        pltpu.VMEM(shape, BF16)
        for shape in shapes[1:] + [(depth, key_width), (local_tokens, depth), (local_tokens, key_width)]
    ]
    results = pl.pallas_call(
        functools.partial(kernel, names, owners, slots, 1.0 / math.sqrt(total_tokens)),
        in_specs=[hbm] * 5,
        out_specs=[vmem] * len(kept),
        out_shape=kept,
        scratch_shapes=list(scratch.values()),
        compiler_params=pltpu.CompilerParams(
            collective_id=0, has_side_effects=True, vmem_limit_bytes=44 * 1024 * 1024
        ),
    )(*[
        pltpu.with_memory_space_constraint(v, pltpu.HBM)
        for v in (counts, scales, block_codes, tokens, cotangent)
    ])
    return tuple(pl.pallas_call(
        functools.partial(last_kernel, planes),
        in_specs=[vmem] * len(kept),
        out_specs=[hbm] * 3,
        out_shape=[pltpu.HBM(shape, BF16) for shape in shapes],
        scratch_shapes=[
            pltpu.VMEM(shapes[0], BF16), pltpu.VMEM((local_tokens, depth), BF16), dma((CHUNKS + 2,))
        ],
        compiler_params=pltpu.CompilerParams(vmem_limit_bytes=16 * 1024 * 1024),
    )(*[pltpu.with_memory_space_constraint(v, pltpu.VMEM) for v in results]))


def solution(mesh):
    return jax.shard_map(
        body,
        mesh=mesh,
        in_specs=(
            P(("dp", "fsdp"), None),
            P("fsdp", None, None),
            P("fsdp"),
            P(),
            P(("dp", "fsdp"), None),
        ),
        out_specs=(P(("dp", "fsdp"), None), P(("dp", "fsdp"), None), P("fsdp", None, None)),
        check_vma=False,
    )
```
